8 devices in a mesh: data: 8 (over z, y, x, core).
Axes of the slice: x: 2, y: 2, z: 1, core: 2. Of those that a mesh axis runs over, the one named last changes fastest.
Arguments:
- x_in: bfloat16 [16384, 2048], P('data')
- dy_in: bfloat16 [16384, 2048], P('data')
- weights: bfloat16 [4, 2048, 2048], replicated
- a_old: float32 [8192, 2048], P('data')
- s_old: float32 [8192, 2048], P('data')
- a_inv: float32 [8192, 2048], P('data')
- s_inv: float32 [4, 2048, 2048], replicated
Outputs:
- output 1: float32 [4, 2048, 2048], replicated
- output 2: float32 [8192, 2048], P('data')
- output 3: float32 [8192, 2048], P('data')
All inputs are finite; a program needn't handle non-finite values.
Results may differ from the reference program's by a relative error of at most 0.001.
Values are sent between devices in bfloat16 or wider.
A program may use at most 1 GiB of HBM per device.

```python
import functools
import jax
import jax.numpy as jnp

D = 2048
LAYERS = 4
TOKENS = 2048
SHARDS = 8
LOW_RANK = 64
BATCH_TOTAL = TOKENS * SHARDS
FACTOR_DECAY = 0.75


def spd_stack(rng_key, base_diag, gram_scale):
    low_rank = jax.random.normal(rng_key, (LAYERS, D, LOW_RANK), jnp.float32)
    gram_mat = jnp.einsum("lir,ljr->lij", low_rank, low_rank)
    gram_mat = 0.5 * (gram_mat + jnp.swapaxes(gram_mat, 1, 2))
    return gram_scale * gram_mat + base_diag * jnp.eye(D, dtype=jnp.float32)


def shard_rows(rng_key, spread):
    key_raw, key_mean, key_scale = jax.random.split(rng_key, 3)
    raw_rows = jax.random.normal(key_raw, (SHARDS, TOKENS, D), jnp.float32)
    offset = 0.7 * jax.random.normal(key_mean, (SHARDS, 1, D), jnp.float32)
    row_scale = jnp.exp(spread * jax.random.normal(key_scale, (SHARDS, 1, 1), jnp.float32))
    return ((raw_rows + offset) * row_scale).reshape(BATCH_TOTAL, D).astype(jnp.bfloat16)


def setup_inputs(seed: int = 0) -> dict:
    key_list = jax.random.split(jax.random.key(seed), 7)
    weights = jax.random.normal(key_list[2], (LAYERS, D, D), jnp.float32) * D ** -0.5
    inv_scale = (LOW_RANK * D) ** -0.5
    return {
        "x_in": shard_rows(key_list[0], 0.5),
        "dy_in": shard_rows(key_list[1], 0.5),
        "weights": weights.astype(jnp.bfloat16),
        "a_old": spd_stack(key_list[3], 0.5, 1.0 / LOW_RANK).reshape(LAYERS * D, D),
        "s_old": spd_stack(key_list[4], 0.5, 1.0 / LOW_RANK).reshape(LAYERS * D, D),
        "a_inv": spd_stack(key_list[5], 0.5, inv_scale).reshape(LAYERS * D, D),
        "s_inv": spd_stack(key_list[6], 0.5, inv_scale),
    }


def gelu_grad(pre_act, d_act):
    pullback = jax.vjp(functools.partial(jax.nn.gelu, approximate=True), pre_act.astype(jnp.float32))[1]
    return pullback(d_act.astype(jnp.float32))[0].astype(jnp.bfloat16)


def reference(x_in, dy_in, weights, a_old, s_old, a_inv, s_inv):
    layer_inputs = [x_in]
    pre_acts = []
    for layer_id in range(LAYERS - 1):
        pre_act = jnp.dot(layer_inputs[layer_id], weights[layer_id], preferred_element_type=jnp.float32).astype(jnp.bfloat16)
        pre_acts.append(pre_act)
        layer_inputs.append(jax.nn.gelu(pre_act.astype(jnp.float32), approximate=True).astype(jnp.bfloat16))
    out_grads = [dy_in] * LAYERS
    for layer_id in range(LAYERS - 1, 0, -1):
        d_act = jnp.dot(out_grads[layer_id], weights[layer_id].T, preferred_element_type=jnp.float32).astype(jnp.bfloat16)
        out_grads[layer_id - 1] = gelu_grad(pre_acts[layer_id - 1], d_act)
    a_facs = []
    s_facs = []
    updates = []
    for layer_id in range(LAYERS):
        h_in = layer_inputs[layer_id]
        g_out = out_grads[layer_id]
        a_facs.append(jnp.dot(h_in.T, h_in, preferred_element_type=jnp.float32) / BATCH_TOTAL)
        s_facs.append(jnp.dot(g_out.T, g_out, preferred_element_type=jnp.float32) / BATCH_TOTAL)
        w_grad = jnp.dot(h_in.T, g_out, preferred_element_type=jnp.float32) / BATCH_TOTAL
        a_inv_layer = a_inv[layer_id * D:(layer_id + 1) * D]
        updates.append(jnp.dot(a_inv_layer, jnp.dot(w_grad, s_inv[layer_id])))
    a_new = FACTOR_DECAY * a_old + (1.0 - FACTOR_DECAY) * jnp.concatenate(a_facs, axis=0)
    s_new = FACTOR_DECAY * s_old + (1.0 - FACTOR_DECAY) * jnp.concatenate(s_facs, axis=0)
    return (jnp.stack(updates), a_new, s_new)
```

```python
import functools
import jax
import jax.numpy as jnp
from jax import lax
from jax.experimental import pallas as pl
from jax.sharding import PartitionSpec as P


FACTOR_DECAY = 0.75
PRECISE = lax.Precision.HIGHEST
HALF_TOP = 32768.0
WIRE = jnp.float16


def gelu_grad(pre_act, d_act):
    pullback = jax.vjp(functools.partial(jax.nn.gelu, approximate=True), pre_act.astype(jnp.float32))[1]
    return pullback(d_act.astype(jnp.float32))[0].astype(jnp.bfloat16)


def cross_rows(left_op, right_op):
    return jnp.einsum("bi,bj->ij", left_op, right_op, preferred_element_type=jnp.float32)


def peak(val):
    return jnp.max(jnp.abs(val)).astype(jnp.float32)


def solution(mesh):
    n_dev = mesh.shape["data"]
    pairs = [[p, p + 1] for p in range(0, n_dev, 2)]

    def hop(val, mask):
        return lax.ppermute(val, "data", [(p, p ^ mask) for p in range(n_dev)])

    def pair_rows(val):
        return lax.all_gather(val, "data", axis_index_groups=pairs, axis=0, tiled=True)

    def device_step(x_loc, dy_loc, weights, a_old_rows, s_old_rows, a_inv_rows, s_inv):
        n_layers, width = weights.shape[0], weights.shape[1]
        batch_total = x_loc.shape[0] * n_dev
        own = a_old_rows.shape[0]
        half = own // 2
        me = lax.axis_index("data")
        chip, core = me // 2, me % 2

        def after(val, *done):
            return lax.optimization_barrier((val,) + done)[0]

        def everywhere(top):
            for mask in (1, 2, 4):
                top = jnp.maximum(top, hop(top, mask))
            return top

        def scale_of(left, right):
            return HALF_TOP / jnp.clip(left * right, 1e-30, 3e38)

        def forward(act, weight):
            pre = jnp.dot(act, weight, preferred_element_type=jnp.float32).astype(jnp.bfloat16)
            act = jax.nn.gelu(pre.astype(jnp.float32), approximate=True).astype(jnp.bfloat16)
            return lax.optimization_barrier((pre, act, peak(act)))

        def backward(grad, weight, pre):
            d_act = jnp.einsum("bj,ij->bi", grad, weight, preferred_element_type=jnp.float32).astype(jnp.bfloat16)
            grad = gelu_grad(pre, d_act)
            return lax.optimization_barrier((grad, peak(grad)))

        def product(left, right, first, rows):
            lhs = lax.dynamic_slice(left, (0, core * own + first), (left.shape[0], rows))
            return cross_rows(lhs, right)

        def chosen(vals, rels):
            def branch(k, vals):
                return tuple(vals[k ^ rel] for rel in rels)

            return lax.switch(chip, [functools.partial(branch, k) for k in range(n_layers)], vals)

        def gathered(vals, rels):
            return {rel: pair_rows(val) for rel, val in zip(rels, lax.optimization_barrier(vals))}

        def partial_sum(operands, scales, rel, first, rows, arrived, done):
            scale = after(scales[chip ^ rel] / batch_total, *done)
            out = product(operands[0][rel], operands[1][rel], first, rows) * scale
            for part in arrived:
                out = out + part.astype(jnp.float32)
            return lax.optimization_barrier(out.astype(WIRE))

        class Routes:
            def __init__(self, operands, scales):
                self.operands, self.scales = operands, scales

            def opposite(self, *done):
                sent_x = partial_sum(self.operands, self.scales, 3, 0, half, (), done)
                sent_y = partial_sum(self.operands, self.scales, 3, half, half, (), (sent_x,))
                self.mid_x, self.mid_y = hop(sent_x, 2), hop(sent_y, 4)
                return sent_y

            def direct(self, *done):
                sent_x = partial_sum(self.operands, self.scales, 1, 0, half, (), done)
                sent_y = partial_sum(self.operands, self.scales, 2, half, half, (), (sent_x,))
                self.near_x, self.near_y = hop(sent_x, 2), hop(sent_y, 4)
                return sent_y

            def joined(self, *done):
                sent_y = partial_sum(self.operands, self.scales, 2, 0, half, (self.mid_x,), done)
                sent_x = partial_sum(self.operands, self.scales, 1, half, half, (self.mid_y,), (sent_y,))
                far_x, far_y = hop(sent_y, 4), hop(sent_x, 2)
                self.parts = ((self.near_x, far_x), (self.near_y, far_y))
                return sent_x

            def whole(self, rel, mask, arrived, *done):
                sent = partial_sum(self.operands, self.scales, rel, 0, own, arrived, done)
                return sent, hop(sent, mask)

            def final(self, old, *done):
                inv = after(1.0 / self.scales[chip], *done)
                wire = [near.astype(jnp.float32) + far.astype(jnp.float32) for near, far in self.parts]
                wire = jnp.concatenate(wire, axis=0) if len(wire) > 1 else wire[0]
                mean = product(self.operands[0][0], self.operands[1][0], 0, own) / batch_total + wire * inv
                if old is not None:
                    mean = FACTOR_DECAY * old + (1.0 - FACTOR_DECAY) * mean
                return lax.optimization_barrier(mean)

        h_peaks = [peak(x_loc)]
        pre_1, act_1, top = forward(x_loc, weights[0])
        h_peaks.append(top)
        pre_2, act_2, top = forward(act_1, weights[1])
        h_peaks.append(top)
        w3_norm = jnp.max(jnp.sum(jnp.abs(weights[2].astype(jnp.float32)), axis=0))
        w2_norm = jnp.max(jnp.sum(jnp.abs(weights[1].astype(jnp.float32)), axis=1))
        h_top = everywhere(jnp.stack(h_peaks))
        h_top = jnp.append(h_top, 1.1 * h_top[2] * w3_norm)
        pre_3, act_3, _ = forward(act_2, weights[2])
        order = (3, 1, 2, 0)
        h_rot = gathered(chosen((x_loc, act_1, act_2, act_3), order), order)
        routes_a = Routes((h_rot, h_rot), scale_of(h_top, h_top))

        g_peaks = [peak(dy_loc)]
        grad_3, top = backward(after(dy_loc, act_3), weights[3], pre_3)
        g_peaks.append(top)
        done, mid = routes_a.whole(3, 2, (), grad_3)
        grad_2, top = backward(after(grad_3, done), weights[2], pre_2)
        g_peaks.append(top)
        g_top = everywhere(jnp.stack(g_peaks[::-1]))
        g_top = jnp.concatenate([(1.25 * g_top[0] * w2_norm)[None], g_top])
        done, near = routes_a.whole(1, 2, (), grad_2)
        grad_1, _ = backward(after(grad_2, done), weights[1], pre_1)
        first_rot = chosen((grad_1, grad_2, grad_3, dy_loc), (3,))
        g_rot = gathered(first_rot, (3,))
        done, far = routes_a.whole(2, 4, (mid,), first_rot[0])
        routes_a.parts = ((near, far),)
        g_rot.update(gathered(chosen(after((grad_1, grad_2, grad_3, dy_loc), done), order[1:]), order[1:]))

        routes_g = Routes((h_rot, g_rot), scale_of(h_top, g_top))
        routes_s = Routes((g_rot, g_rot), scale_of(g_top, g_top))
        done = routes_g.opposite(done)
        done = routes_g.direct(done)
        a_new = routes_a.final(a_old_rows, done)
        done = routes_g.joined(a_new)
        done = routes_s.opposite(done)
        done = routes_s.direct(done)
        g_sum = routes_g.final(None, done)
        s_inv_own = lax.dynamic_index_in_dim(s_inv, chip, axis=0, keepdims=False)
        right = jnp.dot(g_sum, s_inv_own, precision=PRECISE)
        right_other = hop(right, 1)
        done = routes_s.joined(right)

        def encode(val):
            top = jnp.clip(jnp.max(jnp.abs(val)), 1e-30, 3e38)
            power = jnp.clip(jnp.ceil(jnp.log2(top)), -100.0, 128.0)
            code = (val * jnp.exp2(15.0 - power)).astype(WIRE)
            return jnp.concatenate([code, jnp.full((16, width), power, WIRE)], axis=0)

        def blank_kernel(out_ref):
            pass

        u_full = pl.pallas_call(
            blank_kernel,
            out_shape=jax.ShapeDtypeStruct((n_layers, width, width), jnp.float32),
            out_specs=pl.BlockSpec(memory_space=pl.ANY),
        )()

        def place(u_full, part, rel, which, first):
            power = part[half, 0].astype(jnp.float32)
            val = (part[:half].astype(jnp.float32) * jnp.exp2(power - 15.0))[None]
            return lax.dynamic_update_slice(u_full, val, (chip ^ rel, which * own + first, 0))

        coded, prev = [], done
        for first in (0, half):
            inv_own = lax.dynamic_slice(a_inv_rows, (first, core * own), (half, own))
            inv_other = lax.dynamic_slice(a_inv_rows, (first, (1 - core) * own), (half, own))
            u_piece = jnp.dot(inv_own, after(right, prev), precision=PRECISE)
            u_piece = u_piece + jnp.dot(inv_other, after(right_other, u_piece), precision=PRECISE)
            prev = encode(u_piece)
            coded.append(prev)
        from_x = [hop(part, 2) for part in coded]
        from_y = [hop(part, 4) for part in coded]
        diag = [hop(from_x[0], 4), hop(from_y[1], 2)]
        s_new = routes_s.final(s_old_rows, prev)
        for parts, rel in ((coded, 0), (from_x, 1), (from_y, 2), (diag, 3)):
            for part, first in zip(parts, (0, half)):
                u_full = place(u_full, part, rel, core, first)
                u_full = place(u_full, hop(part, 1), rel, 1 - core, first)
        return u_full, a_new, s_new

    row_spec = P("data", None)
    return jax.shard_map(
        device_step,
        mesh=mesh,
        in_specs=(row_spec, row_spec, P(), row_spec, row_spec, row_spec, P()),
        out_specs=(P(), row_spec, row_spec),
        check_vma=False,
    )
```

```python
import functools
import jax
import jax.numpy as jnp
from jax import lax
from jax.experimental import pallas as pl
from jax.experimental.pallas import tpu as pltpu
from jax.sharding import PartitionSpec as P


FACTOR_DECAY = 0.75
PRECISE = lax.Precision.HIGHEST
HALF_TOP = 32768.0
WIRE = jnp.float16
GELU_C, GELU_A = (2.0 / 3.141592653589793) ** 0.5, 0.044715
PARTS, SLOTS = 4, 8


def gelu_grad(pre_act, d_act):
    z = pre_act.astype(jnp.float32)
    cubic = (GELU_C * GELU_A) * (z * z)
    tanh = jnp.tanh(z * (cubic + GELU_C))
    slope = 3.0 * cubic + GELU_C
    return (d_act.astype(jnp.float32) * (0.5 + 0.5 * (tanh + z * (slope - tanh * tanh * slope)))).astype(jnp.bfloat16)


def cross_rows(left_op, right_op):
    return jnp.einsum("bi,bj->ij", left_op, right_op, preferred_element_type=jnp.float32)


def peak(val):
    return jnp.max(jnp.abs(val)).astype(jnp.float32)


def solution(mesh):
    n_dev = mesh.shape["data"]
    pairs = [[p, p + 1] for p in range(0, n_dev, 2)]

    def hop(val, mask):
        return lax.ppermute(val, "data", [(p, p ^ mask) for p in range(n_dev)])

    def pair_rows(val):
        return lax.all_gather(val, "data", axis_index_groups=pairs, axis=0, tiled=True)

    def device_step(x_loc, dy_loc, weights, a_old_rows, s_old_rows, a_inv_rows, s_inv):
        n_layers, width = weights.shape[0], weights.shape[1]
        batch_total = x_loc.shape[0] * n_dev
        own = a_old_rows.shape[0]
        half = own // 2
        me = lax.axis_index("data")
        chip, core = me // 2, me % 2

        def after(val, *done):
            return lax.optimization_barrier((val,) + done)[0]

        def everywhere(top):
            for mask in (1, 2, 4):
                top = jnp.maximum(top, hop(top, mask))
            return top

        def scale_of(left, right):
            return HALF_TOP / jnp.clip(left * right, 1e-30, 3e38)

        def forward(act, weight):
            pre = jnp.dot(act, weight, preferred_element_type=jnp.float32).astype(jnp.bfloat16)
            act = jax.nn.gelu(pre.astype(jnp.float32), approximate=True).astype(jnp.bfloat16)
            return lax.optimization_barrier((pre, act, peak(act)))

        def backward(grad, weight, pre):
            d_act = jnp.einsum("bj,ij->bi", grad, weight, preferred_element_type=jnp.float32).astype(jnp.bfloat16)
            grad = gelu_grad(pre, d_act)
            return lax.optimization_barrier((grad, peak(grad)))

        def product(left, right, first, rows):
            lhs = lax.dynamic_slice(left, (0, core * own + first), (left.shape[0], rows))
            return cross_rows(lhs, right)

        def chosen(vals, rels):
            rows = vals[0].shape[0] // PARTS
            work = [(rel, out, part) for out, rel in enumerate(rels) for part in range(PARTS)]

            def kernel(*refs):
                ins, outs = refs[:n_layers], refs[n_layers:n_layers + len(rels)]
                buf, in_sem, out_sem = refs[n_layers + len(rels):]
                here = lax.axis_index("data") // 2

                def fetch(n):
                    rel, _, part = work[n]
                    slot = n % SLOTS
                    for k in range(n_layers):
                        @pl.when(here == k)
                        def _():
                            src = ins[k ^ rel].at[pl.ds(part * rows, rows)]
                            pltpu.make_async_copy(src, buf.at[slot], in_sem.at[slot]).start()

                def leave(n):
                    _, out, part = work[n]
                    slot = n % SLOTS
                    return pltpu.make_async_copy(buf.at[slot], outs[out].at[pl.ds(part * rows, rows)], out_sem.at[slot])

                ahead = SLOTS // 2
                for n in range(len(work) + ahead):
                    if n < len(work):
                        if n >= SLOTS:
                            leave(n - SLOTS).wait()
                        fetch(n)
                    if n >= ahead:
                        slot = (n - ahead) % SLOTS
                        pltpu.make_async_copy(ins[0].at[pl.ds(0, rows)], buf.at[slot], in_sem.at[slot]).wait()
                        leave(n - ahead).start()
                for n in range(max(len(work) - SLOTS, 0), len(work)):
                    leave(n).wait()

            shape = jax.ShapeDtypeStruct(vals[0].shape, vals[0].dtype)
            any_spec = pl.BlockSpec(memory_space=pl.ANY)
            size = vals[0].size * 2
            return pl.pallas_call(
                kernel,
                out_shape=(shape,) * len(rels),
                in_specs=[any_spec] * n_layers,
                out_specs=(any_spec,) * len(rels),
                scratch_shapes=[
                    pltpu.VMEM((SLOTS, rows, vals[0].shape[1]), vals[0].dtype),
                    pltpu.SemaphoreType.DMA((SLOTS,)),
                    pltpu.SemaphoreType.DMA((SLOTS,)),
                ],
                cost_estimate=pl.CostEstimate(flops=size * len(rels) * 8, bytes_accessed=2 * size * len(rels), transcendentals=0),
            )(*vals)

        def gathered(vals, rels):
            return {rel: pair_rows(val) for rel, val in zip(rels, lax.optimization_barrier(vals))}

        def partial_sum(operands, scales, rel, first, rows, arrived, done):
            scale = after(scales[chip ^ rel] / batch_total, *done)
            out = product(operands[0][rel], operands[1][rel], first, rows) * scale
            for part in arrived:
                out = out + part.astype(jnp.float32)
            return lax.optimization_barrier(out.astype(WIRE))

        class Routes:
            def __init__(self, operands, scales):
                self.operands, self.scales = operands, scales

            def opposite(self, *done):
                sent_x = partial_sum(self.operands, self.scales, 3, 0, half, (), done)
                sent_y = partial_sum(self.operands, self.scales, 3, half, half, (), (sent_x,))
                self.mid_x, self.mid_y = hop(sent_x, 2), hop(sent_y, 4)
                return sent_y

            def direct(self, *done, between=None):
                sent_x = partial_sum(self.operands, self.scales, 1, 0, half, (), done)
                self.near_x = hop(sent_x, 2)
                filled = between(sent_x) if between else sent_x
                sent_y = partial_sum(self.operands, self.scales, 2, half, half, (), (filled,))
                self.near_y = hop(sent_y, 4)
                return sent_y, filled

            def joined(self, *done):
                sent_y = partial_sum(self.operands, self.scales, 2, 0, half, (self.mid_x,), done)
                sent_x = partial_sum(self.operands, self.scales, 1, half, half, (self.mid_y,), (sent_y,))
                far_x, far_y = hop(sent_y, 4), hop(sent_x, 2)
                self.parts = ((self.near_x, far_x), (self.near_y, far_y))
                return sent_x

            def whole(self, rel, mask, arrived, *done):
                sent = partial_sum(self.operands, self.scales, rel, 0, own, arrived, done)
                return sent, hop(sent, mask)

            def final(self, old, *done):
                inv = after(1.0 / self.scales[chip], *done)
                wire = [near.astype(jnp.float32) + far.astype(jnp.float32) for near, far in self.parts]
                wire = jnp.concatenate(wire, axis=0) if len(wire) > 1 else wire[0]
                mean = product(self.operands[0][0], self.operands[1][0], 0, own) / batch_total + wire * inv
                if old is not None:
                    mean = FACTOR_DECAY * old + (1.0 - FACTOR_DECAY) * mean
                return lax.optimization_barrier(mean)

        h_peaks = [peak(x_loc)]
        pre_1, act_1, top = forward(x_loc, weights[0])
        h_peaks.append(top)
        pre_2, act_2, top = forward(act_1, weights[1])
        h_peaks.append(top)
        w3_norm = jnp.max(jnp.sum(jnp.abs(weights[2].astype(jnp.float32)), axis=0))
        w2_norm = jnp.max(jnp.sum(jnp.abs(weights[1].astype(jnp.float32)), axis=1))
        h_top = everywhere(jnp.stack(h_peaks))
        h_top = jnp.append(h_top, 1.1 * h_top[2] * w3_norm)
        pre_3, act_3, _ = forward(act_2, weights[2])
        order = (3, 1, 2, 0)
        h_vals = (x_loc, act_1, act_2, act_3)
        first_h = chosen(h_vals, (3,))
        h_rot = gathered(first_h, (3,))
        routes_a = Routes((h_rot, h_rot), scale_of(h_top, h_top))

        g_peaks = [peak(dy_loc)]
        grad_3, top = backward(after(dy_loc, act_3), weights[3], pre_3)
        g_peaks.append(top)
        done, mid = routes_a.whole(3, 2, (), grad_3)
        h_rot.update(gathered(chosen(after(h_vals, done), order[1:]), order[1:]))
        grad_2, top = backward(after(grad_3, done), weights[2], pre_2)
        g_peaks.append(top)
        g_top = everywhere(jnp.stack(g_peaks[::-1]))
        g_top = jnp.concatenate([(1.25 * g_top[0] * w2_norm)[None], g_top])
        done, near = routes_a.whole(1, 2, (), grad_2)
        grad_1, _ = backward(after(grad_2, done), weights[1], pre_1)
        first_rot = chosen((grad_1, grad_2, grad_3, dy_loc), (3,))
        g_rot = gathered(first_rot, (3,))
        done, far = routes_a.whole(2, 4, (mid,), first_rot[0])
        routes_a.parts = ((near, far),)
        g_rot.update(gathered(chosen(after((grad_1, grad_2, grad_3, dy_loc), done), order[1:]), order[1:]))

        routes_g = Routes((h_rot, g_rot), scale_of(h_top, g_top))
        routes_s = Routes((g_rot, g_rot), scale_of(g_top, g_top))
        done = routes_g.opposite(done)
        done, a_new = routes_g.direct(done, between=functools.partial(routes_a.final, a_old_rows))
        done = routes_g.joined(done)
        done = routes_s.opposite(done)
        done, _ = routes_s.direct(done)
        g_sum = routes_g.final(None, done)
        s_inv_own = lax.dynamic_index_in_dim(s_inv, chip, axis=0, keepdims=False)
        right = jnp.dot(g_sum, s_inv_own, precision=PRECISE)
        right_other = hop(right, 1)
        done = routes_s.joined(right)

        def encode(val):
            top = jnp.clip(jnp.max(jnp.abs(val)), 1e-30, 3e38)
            power = jnp.clip(jnp.ceil(jnp.log2(top)), -100.0, 128.0)
            code = (val * jnp.exp2(15.0 - power)).astype(WIRE)
            return jnp.concatenate([code, jnp.full((16, width), power, WIRE)], axis=0)

        def blank_kernel(out_ref):
            pass

        u_full = pl.pallas_call(
            blank_kernel,
            out_shape=jax.ShapeDtypeStruct((n_layers, width, width), jnp.float32),
            out_specs=pl.BlockSpec(memory_space=pl.ANY),
        )()

        def place(u_full, part, rel, which, first):
            back = jnp.exp2(part[half:half + 1].astype(jnp.float32) - 15.0)
            val = (part[:half].astype(jnp.float32) * back)[None]
            return lax.dynamic_update_slice(u_full, val, (chip ^ rel, which * own + first, 0))

        coded, prev = [], done
        for first in (0, half):
            inv_own = lax.dynamic_slice(a_inv_rows, (first, core * own), (half, own))
            inv_other = lax.dynamic_slice(a_inv_rows, (first, (1 - core) * own), (half, own))
            u_piece = jnp.dot(inv_own, after(right, prev), precision=PRECISE)
            u_piece = u_piece + jnp.dot(inv_other, after(right_other, u_piece), precision=PRECISE)
            prev = encode(u_piece)
            coded.append(prev)
        from_x = [hop(part, 2) for part in coded]
        from_y = [hop(part, 4) for part in coded]
        diag = [hop(from_x[0], 4), hop(from_y[1], 2)]
        s_new = routes_s.final(s_old_rows, prev)
        for parts, rel in ((coded, 0), (from_x, 1), (from_y, 2), (diag, 3)):
            for part, first in zip(parts, (0, half)):
                u_full = place(u_full, part, rel, core, first)
                u_full = place(u_full, hop(part, 1), rel, 1 - core, first)
        return u_full, a_new, s_new

    row_spec = P("data", None)
    return jax.shard_map(
        device_step,
        mesh=mesh,
        in_specs=(row_spec, row_spec, P(), row_spec, row_spec, row_spec, P()),
        out_specs=(P(), row_spec, row_spec),
        check_vma=False,
    )
```

```python
import jax
import jax.numpy as jnp
from jax import lax
from jax.experimental import pallas as pl
from jax.experimental.pallas import tpu as pltpu
from jax.sharding import PartitionSpec as P


FACTOR_DECAY = 0.75
PRECISE = lax.Precision.HIGHEST
HALF_TOP = 32768.0
WIRE = jnp.float16
GELU_C, GELU_A = (2.0 / 3.141592653589793) ** 0.5, 0.044715
PARTS, SLOTS = 8, 16


def gelu_grad(pre_act, d_act):
    z = pre_act.astype(jnp.float32)
    cubic = (GELU_C * GELU_A) * (z * z)
    tanh = jnp.tanh(z * (cubic + GELU_C))
    slope = 3.0 * cubic + GELU_C
    return (d_act.astype(jnp.float32) * (0.5 + 0.5 * (tanh + z * (slope - tanh * tanh * slope)))).astype(jnp.bfloat16)


def cross_rows(left_op, right_op):
    return jnp.einsum("bi,bj->ij", left_op, right_op, preferred_element_type=jnp.float32)


def peak(val):
    return jnp.max(jnp.abs(val)).astype(jnp.float32)


def solution(mesh):
    n_dev = mesh.shape["data"]
    pairs = [[p, p + 1] for p in range(0, n_dev, 2)]

    def hop(val, mask):
        return lax.ppermute(val, "data", [(p, p ^ mask) for p in range(n_dev)])

    def pair_rows(val):
        return lax.all_gather(val, "data", axis_index_groups=pairs, axis=0, tiled=True)

    def device_step(x_loc, dy_loc, weights, a_old_rows, s_old_rows, a_inv_rows, s_inv):
        n_layers, width = weights.shape[0], weights.shape[1]
        batch_total = x_loc.shape[0] * n_dev
        own = a_old_rows.shape[0]
        half = own // 2
        me = lax.axis_index("data")
        chip, core = me // 2, me % 2

        def after(val, *done):
            return lax.optimization_barrier((val,) + done)[0]

        def everywhere(top):
            for mask in (1, 2, 4):
                top = jnp.maximum(top, hop(top, mask))
            return top

        def scale_of(left, right):
            return HALF_TOP / jnp.clip(left * right, 1e-30, 3e38)

        def forward(act, weight):
            pre = jnp.dot(act, weight, preferred_element_type=jnp.float32).astype(jnp.bfloat16)
            act = jax.nn.gelu(pre.astype(jnp.float32), approximate=True).astype(jnp.bfloat16)
            return lax.optimization_barrier((pre, act, peak(act)))

        def backward(grad, weight, pre):
            d_act = jnp.einsum("bj,ij->bi", grad, weight, preferred_element_type=jnp.float32).astype(jnp.bfloat16)
            grad = gelu_grad(pre, d_act)
            return lax.optimization_barrier((grad, peak(grad)))

        def product(left, right, first, cols):
            lhs = lax.dynamic_slice(left, (0, core * own), (left.shape[0], own))
            return cross_rows(lhs, right[:, first:first + cols])

        def chosen(vals, rels):
            rows = vals[0].shape[0] // PARTS
            work = [(rel, out, part) for out, rel in enumerate(rels) for part in range(PARTS)]

            def kernel(*refs):
                ins, outs = refs[:n_layers], refs[n_layers:n_layers + len(rels)]
                buf, in_sem, out_sem = refs[n_layers + len(rels):]
                here = lax.axis_index("data") // 2

                def fetch(n):
                    rel, _, part = work[n]
                    slot = n % SLOTS
                    for k in range(n_layers):
                        @pl.when(here == k)
                        def _():
                            src = ins[k ^ rel].at[pl.ds(part * rows, rows)]
                            pltpu.make_async_copy(src, buf.at[slot], in_sem.at[slot]).start()

                def leave(n):
                    _, out, part = work[n]
                    slot = n % SLOTS
                    return pltpu.make_async_copy(buf.at[slot], outs[out].at[pl.ds(part * rows, rows)], out_sem.at[slot])

                ahead = SLOTS // 2
                for n in range(len(work) + ahead):
                    if n < len(work):
                        if n >= SLOTS:
                            leave(n - SLOTS).wait()
                        fetch(n)
                    if n >= ahead:
                        slot = (n - ahead) % SLOTS
                        pltpu.make_async_copy(ins[0].at[pl.ds(0, rows)], buf.at[slot], in_sem.at[slot]).wait()
                        leave(n - ahead).start()
                for n in range(max(len(work) - SLOTS, 0), len(work)):
                    leave(n).wait()

            shape = jax.ShapeDtypeStruct(vals[0].shape, vals[0].dtype)
            any_spec = pl.BlockSpec(memory_space=pl.ANY)
            size = vals[0].size * 2
            return pl.pallas_call(
                kernel,
                out_shape=(shape,) * len(rels),
                in_specs=[any_spec] * n_layers,
                out_specs=(any_spec,) * len(rels),
                scratch_shapes=[
                    pltpu.VMEM((SLOTS, rows, vals[0].shape[1]), vals[0].dtype),
                    pltpu.SemaphoreType.DMA((SLOTS,)),
                    pltpu.SemaphoreType.DMA((SLOTS,)),
                ],
                cost_estimate=pl.CostEstimate(flops=size * len(rels) * 8, bytes_accessed=2 * size * len(rels), transcendentals=0),
            )(*vals)

        def gathered(vals, rels):
            return {rel: pair_rows(val) for rel, val in zip(rels, lax.optimization_barrier(vals))}

        def partial_sum(operands, scales, rel, first, cols, arrived, done):
            scale = after(scales[chip ^ rel] / batch_total, *done)
            out = product(operands[0][rel], operands[1][rel], first, cols) * scale
            for part in arrived:
                out = out + part.astype(jnp.float32)
            return lax.optimization_barrier(out.astype(WIRE))

        class Routes:
            def __init__(self, operands, scales):
                self.operands, self.scales = operands, scales

            def opposite(self, *done):
                sent_x = partial_sum(self.operands, self.scales, 3, 0, own, (), done)
                sent_y = partial_sum(self.operands, self.scales, 3, own, own, (), (sent_x,))
                self.mid_x, self.mid_y = hop(sent_x, 2), hop(sent_y, 4)
                return sent_y

            def direct(self, *done, between=None):
                sent_x = partial_sum(self.operands, self.scales, 1, 0, own, (), done)
                self.near_x = hop(sent_x, 2)
                filled = between(sent_x) if between else sent_x
                sent_y = partial_sum(self.operands, self.scales, 2, own, own, (), (filled,))
                self.near_y = hop(sent_y, 4)
                return sent_y, filled

            def joined(self, *done):
                sent_y = partial_sum(self.operands, self.scales, 2, 0, own, (self.mid_x,), done)
                sent_x = partial_sum(self.operands, self.scales, 1, own, own, (self.mid_y,), (sent_y,))
                far_x, far_y = hop(sent_y, 4), hop(sent_x, 2)
                self.parts = ((self.near_x, far_x), (self.near_y, far_y))
                return sent_x

            def whole(self, rel, mask, arrived, *done):
                sent = partial_sum(self.operands, self.scales, rel, 0, width, arrived, done)
                return sent, hop(sent, mask)

            def final(self, old, *done):
                inv = after(1.0 / self.scales[chip], *done)
                wire = [near.astype(jnp.float32) + far.astype(jnp.float32) for near, far in self.parts]
                wire = jnp.concatenate(wire, axis=1) if len(wire) > 1 else wire[0]
                mean = product(self.operands[0][0], self.operands[1][0], 0, width) / batch_total + wire * inv
                if old is not None:
                    mean = FACTOR_DECAY * old + (1.0 - FACTOR_DECAY) * mean
                return lax.optimization_barrier(mean)

        h_peaks = [peak(x_loc)]
        pre_1, act_1, top = forward(x_loc, weights[0])
        h_peaks.append(top)
        pre_2, act_2, top = forward(act_1, weights[1])
        h_peaks.append(top)
        w3_norm = jnp.max(jnp.sum(jnp.abs(weights[2].astype(jnp.float32)), axis=0))
        w2_norm = jnp.max(jnp.sum(jnp.abs(weights[1].astype(jnp.float32)), axis=1))
        h_top = everywhere(jnp.stack(h_peaks))
        h_top = jnp.append(h_top, 1.1 * h_top[2] * w3_norm)
        pre_3, act_3, _ = forward(act_2, weights[2])
        order = (3, 1, 2, 0)
        h_vals = (x_loc, act_1, act_2, act_3)
        first_h = chosen(h_vals, (3,))
        h_rot = gathered(first_h, (3,))
        routes_a = Routes((h_rot, h_rot), scale_of(h_top, h_top))

        g_peaks = [peak(dy_loc)]
        grad_3, top = backward(after(dy_loc, act_3), weights[3], pre_3)
        g_peaks.append(top)
        done, mid = routes_a.whole(3, 2, (), grad_3)
        h_rot.update(gathered(chosen(after(h_vals, done), order[1:]), order[1:]))
        grad_2, top = backward(after(grad_3, done), weights[2], pre_2)
        g_peaks.append(top)
        g_top = everywhere(jnp.stack(g_peaks[::-1]))
        g_top = jnp.concatenate([(1.25 * g_top[0] * w2_norm)[None], g_top])
        done, near = routes_a.whole(1, 2, (), grad_2)
        done, far = routes_a.whole(2, 4, (mid,), done)
        routes_a.parts = ((near, far),)
        grad_1, _ = backward(after(grad_2, done), weights[1], pre_1)
        first_rot = chosen((grad_1, grad_2, grad_3, dy_loc), (3,))
        g_rot = gathered(first_rot, (3,))
        done = first_rot[0]
        g_rot.update(gathered(chosen(after((grad_1, grad_2, grad_3, dy_loc), done), order[1:]), order[1:]))

        routes_g = Routes((h_rot, g_rot), scale_of(h_top, g_top))
        routes_s = Routes((g_rot, g_rot), scale_of(g_top, g_top))
        done = routes_g.opposite(done)
        done, _ = routes_g.direct(done)
        done = routes_g.joined(done)
        done = routes_s.opposite(done)
        done, _ = routes_s.direct(done)
        g_sum = routes_g.final(None, done)
        s_inv_own = lax.dynamic_index_in_dim(s_inv, chip, axis=0, keepdims=False)
        right = jnp.dot(g_sum, s_inv_own, precision=PRECISE)
        right_other = hop(right, 1)
        done = routes_s.joined(right)

        def encode(val):
            top = jnp.clip(jnp.max(jnp.abs(val)), 1e-30, 3e38)
            power = jnp.clip(jnp.ceil(jnp.log2(top)), -100.0, 128.0)
            code = (val * jnp.exp2(15.0 - power)).astype(WIRE)
            return jnp.concatenate([code, jnp.full((16, width), power, WIRE)], axis=0)

        def blank_kernel(out_ref):
            pass

        u_full = pl.pallas_call(
            blank_kernel,
            out_shape=jax.ShapeDtypeStruct((n_layers, width, width), jnp.float32),
            out_specs=pl.BlockSpec(memory_space=pl.ANY),
        )()

        def place(u_full, part, rel, which, first):
            back = jnp.exp2(part[half:half + 1].astype(jnp.float32) - 15.0)
            val = (part[:half].astype(jnp.float32) * back)[None]
            return lax.dynamic_update_slice(u_full, val, (chip ^ rel, which * own + first, 0))

        coded, prev = [], done
        for first in (0, half):
            inv_own = lax.dynamic_slice(a_inv_rows, (first, core * own), (half, own))
            inv_other = lax.dynamic_slice(a_inv_rows, (first, (1 - core) * own), (half, own))
            u_piece = jnp.dot(inv_own, after(right, prev), precision=PRECISE)
            u_piece = u_piece + jnp.dot(inv_other, after(right_other, u_piece), precision=PRECISE)
            prev = encode(u_piece)
            coded.append(prev)
        from_x = [hop(part, 2) for part in coded]
        from_y = [hop(part, 4) for part in coded]
        diag = [hop(from_x[0], 4), hop(from_y[1], 2)]
        s_new = routes_s.final(s_old_rows, prev)
        a_new = routes_a.final(a_old_rows, s_new)
        for parts, rel in ((coded, 0), (from_x, 1), (from_y, 2), (diag, 3)):
            other = [hop(part, 1) for part in parts]
            for part, first in zip(parts, (0, half)):
                u_full = place(u_full, part, rel, core, first)
            for part, first in zip(other, (0, half)):
                u_full = place(u_full, part, rel, 1 - core, first)
        return u_full, a_new, s_new

    row_spec = P("data", None)
    return jax.shard_map(
        device_step,
        mesh=mesh,
        in_specs=(row_spec, row_spec, P(), row_spec, row_spec, row_spec, P()),
        out_specs=(P(), row_spec, row_spec),
        check_vma=False,
    )
```
